512 devices in a mesh: param: 128 (over z, y, core), sensor: 4 (over x).
Axes of the slice: x: 4, y: 4, z: 16, core: 2. Of those that a mesh axis runs over, the one named last changes fastest.
Arguments:
- blocks: bfloat16 [64, 2, 600, 16384], P(None, None, 'sensor', 'param'), may hold values from -0.1875 to 0.1875
- probes: bfloat16 [64, 2, 4, 16384], P(None, None, None, 'param'), may hold values from -6 to 6
Outputs:
- basis: float32 [64, 2, 4, 600], P(None, None, None, 'sensor')
- coeffs: bfloat16 [64, 2, 4, 16384], P('sensor', None, None, 'param')
The draws below stay inside these ranges and needn't reach their ends.
All inputs are finite; a program needn't handle non-finite values.
Results may differ from the reference program's by a relative error of at most 0.0049.
Values sent between devices are 32-bit elements; how exact they have to be, the bound alone decides.
A program may use at most 64 MiB of HBM per device.

```python
import jax
import jax.numpy as jnp
from jax import lax

SENSORS = 600
FREQ_LINES = 64
PROBES = 4
NODES = 16384


def steps_of(own_key, dims, cuts, least, largest):
    loudness = 1.0
    for axis_at, shards_of in cuts:
        draws = jax.random.uniform(jax.random.fold_in(jax.random.fold_in(own_key, 6), axis_at), (shards_of,), jnp.float32, least / len(cuts), largest / len(cuts))
        loudness = loudness * jnp.repeat(jnp.exp(draws), dims[axis_at] // shards_of).reshape((-1,) + (1,) * (len(dims) - 1 - axis_at))
    return loudness


def scatter_about(stream_key, dims, deviation, limit, cuts=(), kind=jnp.bfloat16):
    gain = steps_of(stream_key, dims, cuts, -0.22, 0.18) if cuts else 1.0
    entries = jax.random.normal(stream_key, dims, jnp.float32) * deviation * gain
    return jnp.minimum(jnp.maximum(entries, -limit), limit).astype(kind)


def setup_inputs(seed: int = 0) -> dict:
    key_list = jax.random.split(jax.random.key(seed), 3)
    blocks = scatter_about(key_list[0], (FREQ_LINES, 2, SENSORS, NODES), (2 * SENSORS) ** -0.5, 0.1875, ((2, 4), (3, 128)))
    probes = scatter_about(key_list[1], (FREQ_LINES, 2, PROBES, NODES), 1.0, 6.0, ((3, 128),))
    return {"blocks": blocks, "probes": probes}


def sketch_line(pair):
    block, probe = pair
    block = block.astype(jnp.float32)
    probe = probe.astype(jnp.float32)
    real_part = jnp.einsum('sn,an->as', block[0], probe[0]) - jnp.einsum('sn,an->as', block[1], probe[1])
    imag_part = jnp.einsum('sn,an->as', block[0], probe[1]) + jnp.einsum('sn,an->as', block[1], probe[0])
    return jnp.stack([real_part, imag_part])

def adjoint_line(pair):
    block, vectors = pair
    block = block.astype(jnp.float32)
    vectors = vectors.astype(jnp.float32)
    real_part = jnp.einsum('sn,as->an', block[0], vectors[0]) + jnp.einsum('sn,as->an', block[1], vectors[1])
    imag_part = jnp.einsum('sn,as->an', block[0], vectors[1]) - jnp.einsum('sn,as->an', block[1], vectors[0])
    return jnp.stack([real_part, imag_part])

def reference(blocks, probes):
    sketch = lax.map(sketch_line, (blocks, probes))
    gram = jnp.einsum('fpas,fpbs->ab', sketch, sketch, precision=lax.Precision.HIGHEST) / (2.0 * FREQ_LINES * SENSORS)
    lower = jnp.linalg.cholesky(gram)
    inverse = lax.linalg.triangular_solve(lower, jnp.eye(PROBES, dtype=gram.dtype), left_side=True, lower=True)
    basis = jnp.einsum('ab,fpbs->fpas', inverse, sketch, precision=lax.Precision.HIGHEST)
    rounded = lax.optimization_barrier(basis.astype(jnp.bfloat16))
    coeffs = lax.map(adjoint_line, (blocks, rounded))
    return (basis, coeffs.astype(jnp.bfloat16))
```

```python
import functools

import jax
import jax.numpy as jnp
from jax import lax
from jax.experimental import pallas as pl
from jax.experimental.pallas import tpu as pltpu
from jax.sharding import Mesh
from jax.sharding import PartitionSpec as P

SENSORS = 600
FREQ_LINES = 64
PARAM = ("param_0", "param_1", "param_2")
Z, Y, C, X = 16, 4, 2, 4
MESH = pl.DeviceIdType.MESH
MAIN = 8
TILES = 10
GROUPS = 8
GROUP = 150
TAIL = GROUP - 128
F32 = jnp.float32
BF16 = jnp.bfloat16


def owner_of(tile, c):
    return jnp.where(tile < MAIN, 2 * tile + c, 5 + 8 * (tile - MAIN) - c)


def cholesky_inverse(g):
    low = [[None] * 4 for _ in range(4)]
    inv = [[None] * 4 for _ in range(4)]
    for a in range(4):
        for b in range(a + 1):
            rest = g[a][b]
            for k in range(b):
                rest = rest - low[a][k] * low[b][k]
            low[a][b] = jnp.sqrt(rest) if a == b else rest / low[b][b]
    for b in range(4):
        inv[b][b] = 1.0 / low[b][b]
        for a in range(b + 1, 4):
            total = low[a][b] * inv[b][b]
            for k in range(b + 1, a):
                total = total + low[a][k] * inv[k][b]
            inv[a][b] = -total / low[a][a]
    return inv


def kernel(
    blocks_hbm, probes_hbm, basis_hbm, coef_hbm,
    blk, prb, tmp, part, from_core, ysum, from_y, zsum, from_z, full, gram_in, gram_out, gram_core,
    basis, terms, from_x, coef,
    load_sem, probe_sem, core_send, core_recv, ys_send, ys_recv, zs_send, zs_recv,
    za_send, za_recv, ya_send, ya_recv, ca_send, ca_recv, gx_send, gx_recv, gc_send, gc_recv,
    xs_send, xs_recv, out_sem,
):
    z, y, c, x = (lax.axis_index(n) for n in ("param_0", "param_1", "param_2", "sensor"))
    at = lambda z_, y_, c_, x_: (z_, y_, c_, x_)
    sibling = at(z, y, 1 - c, x)

    pltpu.make_async_copy(probes_hbm, prb, probe_sem).start()

    def load(k):
        g = lax.rem((1 - c) * 4 + k, GROUPS)
        return pltpu.make_async_copy(
            blocks_hbm.at[pl.ds(g * MAIN, MAIN)], blk.at[pl.ds(g * MAIN, MAIN)], load_sem.at[k]
        )

    for k in range(GROUPS):
        load(k).start()
    barrier = pltpu.get_barrier_semaphore()
    for d in range(1, Z):
        pl.semaphore_signal(barrier, inc=1, device_id=at(lax.rem(z + d, Z), y, c, x), device_id_type=MESH)
    for e in range(1, X * Y):
        pl.semaphore_signal(
            barrier, inc=1,
            device_id=at(z, lax.rem(y + e % Y, Y), c, lax.rem(x + e // Y, X)),
            device_id_type=MESH,
        )
    pl.semaphore_signal(barrier, inc=1, device_id=sibling, device_id_type=MESH)

    row = lax.broadcasted_iota(jnp.int32, (8, 128), 0)
    lane = lax.broadcasted_iota(jnp.int32, (8, 128), 1)
    plus = jnp.where(row < 4, -1.0, 1.0).astype(F32)
    tmp[...] = jnp.zeros_like(tmp)
    pltpu.make_async_copy(probes_hbm, prb, probe_sem).wait()

    def sketch_group(k, carry):
        load(k).wait()
        g = lax.rem((1 - c) * 4 + k, GROUPS)
        for q in range(2):
            tails = jnp.zeros((8, 128), F32)
            for j in range(4):
                i = 4 * q + j
                f = g * MAIN + i
                probe = prb[f]
                turned = (plus * pltpu.roll(probe.astype(F32), 4, 0)).astype(BF16)
                left = jnp.concatenate([probe, turned], axis=1)
                right = jnp.concatenate([blk[f, 0], blk[f, 1]], axis=1)
                value = lax.dot_general(
                    left, right, (((1,), (1,)), ((), ())), preferred_element_type=F32
                )
                part[g, i] = value[:, :128]
                tmp[i, :, :GROUP] = value
                tail = tmp[i, :, 128:]
                tails = tails + (tail if j == 0 else pltpu.roll(tail, 32 * j, 1))
            part[g, MAIN + q] = tails
        return carry

    lax.fori_loop(0, GROUPS, sketch_group, 0)
    pl.semaphore_wait(barrier, Z - 1 + X * Y - 1 + 1)

    def to_core(d):
        yy = lax.rem(y + d, Y)
        return pltpu.make_async_remote_copy(
            src_ref=part.at[(1 - c) * 4 + yy], dst_ref=from_core.at[d],
            send_sem=core_send.at[d], recv_sem=core_recv.at[d],
            device_id=sibling, device_id_type=MESH,
        )

    def to_y(d):
        return pltpu.make_async_remote_copy(
            src_ref=ysum.at[d], dst_ref=from_y.at[d],
            send_sem=ys_send.at[d], recv_sem=ys_recv.at[d],
            device_id=at(z, lax.rem(y + d, Y), c, x), device_id_type=MESH,
        )

    for d in (2, 1, 3, 0):
        to_core(d).start()
    for d in (2, 1, 3, 0):
        to_core(d).wait_recv()
        ysum[d] = part[c * 4 + lax.rem(y + d, Y)] + from_core[d]
        if d:
            to_y(d).start()
    for d in (1, 3, 2):
        to_y(d).wait_recv()
    zsum[...] = (ysum[0] + from_y[1]) + (from_y[2] + from_y[3])

    def to_owner(i):
        o = owner_of(i, c)
        d = lax.rem(o - z + Z, Z)
        return d, pltpu.make_async_remote_copy(
            src_ref=zsum.at[i], dst_ref=from_z.at[d],
            send_sem=zs_send.at[i], recv_sem=zs_recv.at[d],
            device_id=at(o, y, c, x), device_id_type=MESH,
        )

    for k in range(TILES):
        d, copy = to_owner(k)

        @pl.when(d != 0)
        def _():
            copy.start()

    is_main = lax.rem(z + c, 2) == 0
    is_tail = lax.rem(z + c, 8) == 5
    mine = jnp.where(is_main, (z - c) // 2, MAIN + (z + c - 5) // 8)
    owns = jnp.logical_or(is_main, is_tail)
    group = c * 4 + y

    def to_ring(d):
        return pltpu.make_async_remote_copy(
            src_ref=full.at[group, mine], dst_ref=full.at[group, mine],
            send_sem=za_send.at[d], recv_sem=za_recv.at[mine],
            device_id=at(lax.rem(z + d, Z), y, c, x), device_id_type=MESH,
        )

    order = [8, 7, 9, 6, 10, 5, 11, 4, 12, 3, 13, 2, 14, 1, 15]

    @pl.when(owns)
    def _():
        total = zsum[mine]
        for d in reversed(order):
            pltpu.make_async_remote_copy(
                src_ref=zsum.at[0], dst_ref=from_z.at[d],
                send_sem=zs_send.at[0], recv_sem=zs_recv.at[d],
                device_id=sibling, device_id_type=MESH,
            ).wait_recv()
            total = total + from_z[d]
        full[group, mine] = total
        for d in order:
            to_ring(d).start()

    for i in range(TILES):
        d, _ = to_owner(i)

        @pl.when(d != 0)
        def _():
            pltpu.make_async_remote_copy(
                src_ref=full.at[group, i], dst_ref=full.at[group, i],
                send_sem=za_send.at[0], recv_sem=za_recv.at[i],
                device_id=sibling, device_id_type=MESH,
            ).wait_recv()

    def to_y_all(d):
        return pltpu.make_async_remote_copy(
            src_ref=full.at[group], dst_ref=full.at[group],
            send_sem=ya_send.at[d], recv_sem=ya_recv.at[d],
            device_id=at(z, lax.rem(y + d, Y), c, x), device_id_type=MESH,
        )

    def to_core_all(d, who):
        g = who * 4 + lax.rem(y - d + Y, Y)
        return pltpu.make_async_remote_copy(
            src_ref=full.at[g], dst_ref=full.at[g],
            send_sem=ca_send.at[d], recv_sem=ca_recv.at[d],
            device_id=sibling, device_id_type=MESH,
        )

    for d in (2, 1, 3):
        to_y_all(d).start()
    to_core_all(0, c).start()

    sums = []
    own = [full[group, i] for i in range(TILES)]
    for k in range(4):
        acc = None
        for tile in own:
            prod = tile * (tile if k == 0 else pltpu.roll(tile, k, 0))
            acc = prod if acc is None else acc + prod
        sums.append(jnp.sum(acc, axis=1, keepdims=True))
    packed = jnp.zeros((8, 128), F32)
    for k in range(4):
        packed = jnp.where(lane == k, sums[k], packed)
    gram_out[...] = packed

    def gram_to(e):
        return pltpu.make_async_remote_copy(
            src_ref=gram_out, dst_ref=gram_in.at[e],
            send_sem=gx_send.at[e], recv_sem=gx_recv.at[e],
            device_id=at(z, lax.rem(y + e % Y, Y), c, lax.rem(x + e // Y, X)), device_id_type=MESH,
        )

    for e in range(1, X * Y):
        gram_to(e).start()
    for d in (1, 3, 2):
        pltpu.make_async_remote_copy(
            src_ref=full.at[group], dst_ref=full.at[c * 4 + lax.rem(y - d + Y, Y)],
            send_sem=ya_send.at[d], recv_sem=ya_recv.at[d],
            device_id=sibling, device_id_type=MESH,
        ).wait_recv()
        to_core_all(d, c).start()
    total = packed
    for e in range(1, X * Y):
        gram_to(e).wait_recv()
        total = total + gram_in[e]
    gram_core[0] = total
    to_gram_core = pltpu.make_async_remote_copy(
        src_ref=gram_core.at[0], dst_ref=gram_core.at[1],
        send_sem=gc_send, recv_sem=gc_recv, device_id=sibling, device_id_type=MESH,
    )
    to_gram_core.start()
    to_gram_core.wait_recv()
    total = total + gram_core[1]
    total = (total + pltpu.roll(total, 4, 0)) / (2.0 * FREQ_LINES * SENSORS)
    g = [[None] * 4 for _ in range(4)]
    for a in range(4):
        for b in range(a + 1):
            picked = jnp.where(jnp.logical_and(row == a, lane == a - b), total, 0.0)
            g[a][b] = jnp.sum(jnp.sum(picked, axis=1, keepdims=True), axis=0, keepdims=True)
    inv = cholesky_inverse(g)
    probe_of = lax.rem(row, 4)
    mix = []
    for k in range(4):
        column = jnp.zeros((8, 128), F32)
        for a in range(k, 4):
            column = jnp.where(probe_of == a, jnp.broadcast_to(inv[a][a - k], (8, 128)), column)
        mix.append(column)

    def mixed(tile):
        out = mix[0] * tile
        for k in range(1, 4):
            out = out + mix[k] * pltpu.roll(tile, k, 0)
        return out

    for d in range(4):
        to_core_all(d, 1 - c).wait_recv()

    minus = -plus

    def to_x(d):
        return pltpu.make_async_remote_copy(
            src_ref=terms.at[d], dst_ref=from_x.at[d],
            send_sem=xs_send.at[d], recv_sem=xs_recv.at[d],
            device_id=at(z, y, c, lax.rem(x + d, X)), device_id_type=MESH,
        )

    for d in (2, 1, 3, 0):
        first = lax.rem(x + d, X) * (FREQ_LINES // X)

        def adjoint_quad(q, carry, d=d, first=first):
            f0 = first + q * 4
            g = f0 // MAIN
            half = lax.rem(q, 2)
            tails = mixed(full[g, MAIN + half])
            for j in range(4):
                f = f0 + j
                main = mixed(full[g, half * 4 + j])
                tail = tails if j == 0 else pltpu.roll(tails, 128 - 32 * j, 1)
                value = jnp.concatenate([main, tail], axis=1)[:, :GROUP]
                basis[f, 0] = value[:4]
                basis[f, 1] = value[4:]
                right = jnp.concatenate([blk[f, 0], blk[f, 1]], axis=1)
                both = jnp.dot(value.astype(BF16), right, preferred_element_type=F32)
                terms[d, q * 4 + j] = both[:, :128] + minus * pltpu.roll(both[:, 128:], 4, 0)
            return carry

        lax.fori_loop(0, FREQ_LINES // X // 4, adjoint_quad, 0)
        if d:
            to_x(d).start()
    basis_out = pltpu.make_async_copy(basis, basis_hbm, out_sem.at[0])
    basis_out.start()
    for d in (1, 3, 2):
        to_x(d).wait_recv()

    def add_up(i, carry):
        coef[i] = ((terms[0, i] + from_x[1, i]) + (from_x[2, i] + from_x[3, i])).astype(BF16)
        return carry

    lax.fori_loop(0, FREQ_LINES // X, add_up, 0)
    coef_out = pltpu.make_async_copy(coef, coef_hbm, out_sem.at[1])
    coef_out.start()

    for d in range(4):
        to_core(d).wait_send()
        to_core_all(d, c).wait_send()
    for d in range(1, 4):
        to_y(d).wait_send()
        to_y_all(d).wait_send()
        to_x(d).wait_send()
    for i in range(TILES):
        d, copy = to_owner(i)

        @pl.when(d != 0)
        def _():
            copy.wait_send()

    @pl.when(owns)
    def _():
        for d in order:
            to_ring(d).wait_send()

    for e in range(1, X * Y):
        gram_to(e).wait_send()
    to_gram_core.wait_send()
    basis_out.wait()
    coef_out.wait()


def on_device(blocks, probes):
    tile = (8, 128)
    dma = pltpu.SemaphoreType.DMA
    basis, coef = pl.pallas_call(
        kernel,
        out_shape=(
            jax.ShapeDtypeStruct((FREQ_LINES, 2, 4, GROUP), F32),
            jax.ShapeDtypeStruct((FREQ_LINES // X, 8, 128), BF16),
        ),
        in_specs=[pl.BlockSpec(memory_space=pl.ANY)] * 2,
        out_specs=(pl.BlockSpec(memory_space=pl.ANY),) * 2,
        scratch_shapes=[
            pltpu.VMEM((FREQ_LINES, 2, GROUP, 128), BF16),
            pltpu.VMEM((FREQ_LINES, 8, 128), BF16),
            pltpu.VMEM((MAIN, 8, 256), F32),
            pltpu.VMEM((GROUPS, TILES, *tile), F32),
            pltpu.VMEM((4, TILES, *tile), F32),
            pltpu.VMEM((4, TILES, *tile), F32),
            pltpu.VMEM((4, TILES, *tile), F32),
            pltpu.VMEM((TILES, *tile), F32),
            pltpu.VMEM((Z, *tile), F32),
            pltpu.VMEM((GROUPS, TILES, *tile), F32),
            pltpu.VMEM((X * Y, *tile), F32),
            pltpu.VMEM(tile, F32),
            pltpu.VMEM((2, *tile), F32),
            pltpu.VMEM((FREQ_LINES, 2, 4, GROUP), F32),
            pltpu.VMEM((X, FREQ_LINES // X, *tile), F32),
            pltpu.VMEM((X, FREQ_LINES // X, *tile), F32),
            pltpu.VMEM((FREQ_LINES // X, *tile), BF16),
            dma((GROUPS,)), dma,
            dma((4,)), dma((4,)),
            dma((4,)), dma((4,)),
            dma((TILES,)), dma((Z,)),
            dma((Z,)), dma((TILES,)),
            dma((4,)), dma((4,)),
            dma((4,)), dma((4,)),
            dma((X * Y,)), dma((X * Y,)),
            dma, dma,
            dma((4,)), dma((4,)),
            dma((2,)),
        ],
        compiler_params=pltpu.CompilerParams(
            collective_id=0, has_side_effects=True, vmem_limit_bytes=48 * 1024 * 1024
        ),
    )(blocks, probes.reshape(FREQ_LINES, 8, 128))
    return basis, coef.reshape(FREQ_LINES // X, 2, 4, 128)


def solution(mesh):
    torus = Mesh(
        mesh.devices.reshape(Z, Y, C, mesh.shape["sensor"]),
        ("param_0", "param_1", "param_2", "sensor"),
    )
    placed = (P(None, None, "sensor", PARAM), P(None, None, None, PARAM))
    return jax.shard_map(
        on_device,
        mesh=torus,
        in_specs=placed,
        out_specs=(P(None, None, None, "sensor"), P("sensor", None, None, PARAM)),
        check_vma=False,
    )
```
